32 devices in a mesh: rows: 8 (over y, x, core), sub: 4 (over z).
Axes of the slice: x: 2, y: 2, z: 4, core: 2. Of those that a mesh axis runs over, the one named last changes fastest.
Arguments:
- u_fem: float32 [120, 524288], P(None, ('rows', 'sub')), may hold values from -600 to 600
- resid_fem: float32 [1, 524288], P(None, ('rows', 'sub')), may hold values from -60 to 60
- slot_map: int32 [32, 32], P(('rows', 'sub')), may hold values from 0 to 31, as said below
- restart: float32 [120, 40], replicated, may hold values from -0.5 to 0.5
- coeff: float32 [3, 120, 120], P(None, None, 'sub'), may hold values from -6 to 6
Outputs:
- new_basis: float32 [40, 524288], P(None, ('rows', 'sub'))
- next_vector: float32 [1, 524288], P(None, ('rows', 'sub'))
- new_coeff: float32 [3, 40, 120], replicated
The draws below stay inside these ranges and needn't reach their ends.
Inputs may be any that keep to these rules, and one draw needn't show every extreme that they name: Each row of slot_map is a permutation of 0 to 31.
All inputs are finite; a program needn't handle non-finite values.
Results may differ from the reference program's by a relative error of at most 0.00015.
Values sent between devices are 32-bit elements; how exact they have to be, the bound alone decides.
A program may use at most 64 MiB of HBM per device.

```python
import math
import jax
import jax.numpy as jnp
from jax import lax

K = 120
KEEP = 40
DEG = 3
M = 120
NDEV = 32
BS = 512
NROWS = 524288


def basis_core(key):
    core_key = jax.random.fold_in(key, 11)
    core = jnp.clip(jax.random.normal(core_key, (K, NROWS), jnp.float32), -5.0, 5.0)
    position = jnp.arange(NROWS, dtype=jnp.float32) / NROWS
    block_scale = jnp.exp(jax.random.uniform(jax.random.fold_in(key, 12), (NROWS // BS,), jnp.float32, math.log(0.5), math.log(2.0)))
    jitter = jax.random.uniform(jax.random.fold_in(key, 13), (NROWS,), jnp.float32, 0.7, 1.3)
    row_scale = (1.0 + 2.0 * position) * jnp.repeat(block_scale, BS) * jitter
    return (core, row_scale)


def draw_u_fem(key, part):
    core, row_scale = basis_core(key)
    width_scale = jnp.exp(jax.random.uniform(jax.random.fold_in(key, 21), (K,), jnp.float32, 0.0, math.log(10.0)))
    mixing = jnp.eye(K, dtype=jnp.float32) + 0.25 * jax.random.normal(jax.random.fold_in(key, 22), (K, K), jnp.float32) / math.sqrt(K)
    mixed = jnp.dot(mixing, core, precision=lax.Precision.HIGHEST)
    values = width_scale[:, None] * mixed * row_scale[None, :]
    return jnp.clip(values, -600.0, 600.0).astype(jnp.float32)


def draw_resid_fem(key, part):
    core, row_scale = basis_core(key)
    weights = jax.random.normal(jax.random.fold_in(key, 31), (K,), jnp.float32) / math.sqrt(K)
    noise = jnp.clip(jax.random.normal(jax.random.fold_in(key, 32), (NROWS,), jnp.float32), -5.0, 5.0)
    values = (jnp.dot(weights, core, precision=lax.Precision.HIGHEST) + noise) * row_scale
    return jnp.clip(values, -60.0, 60.0)[None, :].astype(jnp.float32)


def draw_slot_map(key, part):
    row_keys = jax.random.split(jax.random.fold_in(key, 41), NDEV)
    return jax.vmap(lambda one_key: jax.random.permutation(one_key, NDEV))(row_keys).astype(jnp.int32)


def steps_of(own_key, shape, cuts, least, high):
    def one(dim, parts):
        draws = jax.random.uniform(jax.random.fold_in(jax.random.fold_in(own_key, 6), dim), (parts,), jnp.float32, least / len(cuts), high / len(cuts))
        return jnp.repeat(jnp.exp(draws), shape[dim] // parts).reshape((-1,) + (1,) * (len(shape) - dim - 1))

    gain = one(*cuts[0])
    for cut in cuts[1:]:
        gain = gain * one(*cut)
    return gain


def gaussian(rng, extent, spread, limit, cuts=(), kind=jnp.bfloat16):
    result = spread * jax.random.normal(rng, extent, jnp.float32)
    if cuts:
        result = result * steps_of(rng, extent, cuts, -0.22, 0.18)
    return jnp.clip(result, -limit, limit).astype(kind)


def setup_inputs(seed: int = 0) -> dict:
    seeds = jax.random.split(jax.random.key(seed), 6)
    return {
        "u_fem": draw_u_fem(jax.random.fold_in(seeds[5], 71), 0),
        "resid_fem": draw_resid_fem(jax.random.fold_in(seeds[5], 71), 0),
        "slot_map": draw_slot_map(jax.random.fold_in(seeds[5], 71), 0),
        "restart": gaussian(seeds[3], (K, KEEP), K ** -0.5, 0.5, (), jnp.float32),
        "coeff": gaussian(seeds[4], (DEG, K, M), 1.0, 6.0, ((2, 4),), jnp.float32),
    }


def relayout(values, slot_map):
    width = values.shape[0]
    blocks = values.reshape(width, NDEV, NDEV, BS).transpose(0, 2, 1, 3)
    source = jnp.argsort(slot_map, axis=1).astype(jnp.int32)
    moved = jnp.take_along_axis(blocks, source[None, :, :, None], axis=2)
    return moved.reshape(width, NROWS)

def reference(u_fem, resid_fem, slot_map, restart, coeff):
    highest = lax.Precision.HIGHEST
    gram_sum = jnp.einsum('kn,jn->kj', u_fem, u_fem, precision=highest) / NROWS
    inner_prod = jnp.einsum('kn,n->k', u_fem, resid_fem[0], precision=highest)
    chol_lower = jnp.linalg.cholesky(gram_sum)
    factor = lax.linalg.triangular_solve(chol_lower, restart, left_side=True, lower=True, transpose_a=True)
    new_rows = jnp.einsum('kp,kn->pn', factor, u_fem, precision=highest)
    half_solve = lax.linalg.triangular_solve(chol_lower, inner_prod[:, None], left_side=True, lower=True)
    proj_coef = lax.linalg.triangular_solve(chol_lower, half_solve, left_side=True, lower=True, transpose_a=True)[:, 0] / NROWS
    remainder = resid_fem - jnp.einsum('k,kn->n', proj_coef, u_fem, precision=highest)[None, :]
    norm_sum = jnp.sum(remainder * remainder)
    next_row = remainder * lax.rsqrt(norm_sum / NROWS + 1e-06)
    raised = jnp.dot(chol_lower, restart, precision=highest)
    rotated = jnp.einsum('kp,ikm->ipm', raised, coeff, precision=highest)
    new_coeff = rotated * lax.rsqrt(jnp.mean(rotated * rotated) + 1e-06)
    return (relayout(new_rows, slot_map), relayout(next_row, slot_map), new_coeff)
```

```python
import functools

import jax
import jax.numpy as jnp
from jax import lax
from jax.experimental import pallas as pl
from jax.experimental.pallas import tpu as pltpu

HIGHEST = lax.Precision.HIGHEST
MESH = pl.DeviceIdType.MESH
AXES = ("rows", "sub")
LANES = 128


def round_up(value, unit):
    return -(-value // unit) * unit


def me_of(ns):
    return lax.axis_index("rows") * ns + lax.axis_index("sub")


def greet_all(me, ndev, ns):
    barrier = pltpu.get_barrier_semaphore()

    def greet(o, carry):
        j = (me + o) % ndev
        pl.semaphore_signal(barrier, inc=1, device_id=(j // ns, j % ns), device_id_type=MESH)
        return carry

    lax.fori_loop(1, ndev, greet, 0)
    return barrier


def gram_kernel(ndev, ns, chunk, u_ref, r_ref, out_ref, stage, rs_buf, red, ag_buf, s1, r1, s2, r2):
    me = me_of(ns)
    barrier = greet_all(me, ndev, ns)
    width = out_ref.shape[1]
    pad = width - u_ref.shape[0]
    rpd = width // ndev

    def piece(c, acc):
        cols = pl.ds(pl.multiple_of(c * chunk, chunk), chunk)
        first = lax.broadcasted_iota(jnp.int32, (pad, chunk), 0) == 0
        tail = jnp.where(first, jnp.broadcast_to(r_ref[:, cols], (pad, chunk)), 0.0)
        x = jnp.concatenate([u_ref[:, cols], tail], axis=0)
        hi = x.astype(jnp.bfloat16)
        lo = (x - hi.astype(jnp.float32)).astype(jnp.bfloat16)
        both = jnp.concatenate([hi, lo], axis=0)
        return acc + lax.dot_general(both, both, (((1,), (1,)), ((), ())), preferred_element_type=jnp.float32)

    full = lax.fori_loop(0, u_ref.shape[1] // chunk, piece, jnp.zeros((2 * width, 2 * width), jnp.float32))
    cross = full[:width, width:]
    gram = full[:width, :width] + (cross + cross.T) + full[width:, width:]
    for i in range(ndev):
        stage[i] = gram[i * rpd : (i + 1) * rpd, :]
    rs_buf[me] = stage[me]
    pl.semaphore_wait(barrier, ndev - 1)

    def scatter_copy(j, slot):
        return pltpu.make_async_remote_copy(
            src_ref=stage.at[j], dst_ref=rs_buf.at[slot], send_sem=s1.at[j], recv_sem=r1.at[slot],
            device_id=(j // ns, j % ns), device_id_type=MESH)

    def gather_copy(j, slot):
        return pltpu.make_async_remote_copy(
            src_ref=red, dst_ref=ag_buf.at[slot], send_sem=s2.at[j], recv_sem=r2.at[slot],
            device_id=(j // ns, j % ns), device_id_type=MESH)

    def loop(action):
        def body(o, carry):
            action((me + o) % ndev)
            return carry
        lax.fori_loop(1, ndev, body, 0)

    loop(lambda j: scatter_copy(j, me).start())
    loop(lambda j: scatter_copy(j, j).wait_recv())
    total = jnp.sum(rs_buf[...], axis=0)
    red[...] = total
    ag_buf[me] = total
    loop(lambda j: gather_copy(j, me).start())
    loop(lambda j: gather_copy(j, j).wait_recv())
    for i in range(ndev):
        out_ref[i * rpd : (i + 1) * rpd, :] = ag_buf[i]
    loop(lambda j: scatter_copy(j, me).wait_send())
    loop(lambda j: gather_copy(j, me).wait_send())


def gram_sums(u, r, ndev, ns):
    width = LANES
    rpd = width // ndev
    chunk = min(2048, u.shape[1])
    dma = pltpu.SemaphoreType.DMA((ndev,))
    vmem = pl.BlockSpec(memory_space=pltpu.VMEM)
    return pl.pallas_call(
        functools.partial(gram_kernel, ndev, ns, chunk),
        out_shape=jax.ShapeDtypeStruct((width, width), jnp.float32),
        in_specs=[vmem, vmem],
        out_specs=vmem,
        scratch_shapes=[
            pltpu.VMEM((ndev, rpd, width), jnp.float32),
            pltpu.VMEM((ndev, rpd, width), jnp.float32),
            pltpu.VMEM((rpd, width), jnp.float32),
            pltpu.VMEM((ndev, rpd, width), jnp.float32),
            dma, dma, dma, dma,
        ],
        compiler_params=pltpu.CompilerParams(
            collective_id=0, has_side_effects=True, vmem_limit_bytes=40 * 1024 * 1024),
    )(u, r)


def exchange_kernel(ndev, ns, keep, count, u_ref, r_ref, w_ref, raised_ref, coeff_ref,
                    big_out, small_out, coeff_out, send, small, cg, own_sem,
                    s1, r1, s2, r2, s3, r3):
    r, s = lax.axis_index("rows"), lax.axis_index("sub")
    me = r * ns + s
    nr = ndev // ns
    bs = send.shape[2]
    barrier = greet_all(me, ndev, ns)

    def coeff_copy(t, slot):
        return pltpu.make_async_remote_copy(
            src_ref=coeff_ref, dst_ref=cg.at[slot], send_sem=s3.at[t], recv_sem=r3.at[slot],
            device_id=(r, t), device_id_type=MESH)

    def big_copy(j, slot):
        return pltpu.make_async_remote_copy(
            src_ref=send.at[j], dst_ref=big_out.at[slot], send_sem=s1.at[j], recv_sem=r1.at[slot],
            device_id=(j // ns, j % ns), device_id_type=MESH)

    def small_copy(j, slot):
        return pltpu.make_async_remote_copy(
            src_ref=small.at[j], dst_ref=small_out.at[slot], send_sem=s2.at[j], recv_sem=r2.at[slot],
            device_id=(j // ns, j % ns), device_id_type=MESH)

    def loop(action):
        def body(o, carry):
            action((me + o) % ndev)
            return carry
        lax.fori_loop(1, ndev, body, 0)

    weights = w_ref[...]
    half = ns // 2
    side, pos = s // half, s % half
    across = [(1 - side) * half + (pos + q) % half for q in range(half)]
    beside = [side * half + (pos + q) % half for q in range(half)]
    order = []
    for q in range(half):
        order += [across[q], beside[half - 1 - q]]

    def step(d, acc):
        targets = [((r + d) % nr) * ns + t for t in order]
        for j in targets:
            cols = pl.ds(pl.multiple_of(j * bs, bs), bs)
            y = jnp.dot(weights, u_ref[:, cols], precision=HIGHEST, preferred_element_type=jnp.float32)
            rest = r_ref[:, cols] - y[keep : keep + 1, :]
            send[j] = y[:keep, :]
            small[j, 0:1, :] = rest
            acc = acc + rest * rest

        @pl.when(d == 0)
        def _():
            pl.semaphore_wait(barrier, ndev - 1)

        for j in targets:
            @pl.when(j != me)
            def _():
                big_copy(j, me).start()

        return acc

    acc = lax.fori_loop(0, nr, step, jnp.zeros((1, bs), jnp.float32))
    partial = jnp.sum(acc, axis=1, keepdims=True)

    def mark(j, carry):
        small[j, 1:2, :] = jnp.broadcast_to(partial, (1, bs))
        return carry

    lax.fori_loop(0, ndev, mark, 0)
    own_big = pltpu.make_async_copy(send.at[me], big_out.at[me], own_sem.at[0])
    own_small = pltpu.make_async_copy(small.at[me], small_out.at[me], own_sem.at[1])
    own_big.start()
    own_small.start()
    for o in range(1, ns):
        coeff_copy((s + o) % ns, s).start()
    loop(lambda j: small_copy(j, me).start())
    cg[s] = coeff_ref[...]
    for o in range(1, ns):
        coeff_copy((s + o) % ns, (s + o) % ns).wait_recv()
    turned = [
        lax.dot_general(raised_ref[...], cg[t], (((1,), (1,)), ((), ())), precision=HIGHEST,
                        preferred_element_type=jnp.float32)
        for t in range(ns)
    ]
    squares = sum(jnp.sum(part * part) for part in turned)
    scale = lax.rsqrt(jnp.full((1, 1), squares / count + 1e-06, jnp.float32))
    for t in range(ns):
        coeff_out[t] = turned[t] * scale
    own_big.wait()
    own_small.wait()
    loop(lambda j: big_copy(j, j).wait_recv())
    loop(lambda j: small_copy(j, j).wait_recv())
    loop(lambda j: big_copy(j, me).wait_send())
    loop(lambda j: small_copy(j, me).wait_send())
    for o in range(1, ns):
        coeff_copy((s + o) % ns, s).wait_send()


def exchange(u, r, weights, raised, coeff_t, keep, count, ndev, ns):
    bs = u.shape[1] // ndev
    vmem = pl.BlockSpec(memory_space=pltpu.VMEM)
    hbm = pl.BlockSpec(memory_space=pl.ANY)
    dma = pltpu.SemaphoreType.DMA((ndev,))
    few = pltpu.SemaphoreType.DMA((ns,))
    f32 = jnp.float32
    return pl.pallas_call(
        functools.partial(exchange_kernel, ndev, ns, keep, count),
        out_shape=(
            jax.ShapeDtypeStruct((ndev, keep, bs), f32),
            jax.ShapeDtypeStruct((ndev, 2, bs), f32),
            jax.ShapeDtypeStruct((ns, keep, coeff_t.shape[0]), f32),
        ),
        in_specs=[vmem] * 5,
        out_specs=(hbm, hbm, vmem),
        scratch_shapes=[
            pltpu.VMEM((ndev, keep, bs), f32),
            pltpu.VMEM((ndev, 2, bs), f32),
            pltpu.VMEM((ns,) + coeff_t.shape, f32),
            pltpu.SemaphoreType.DMA((2,)),
            dma, dma, dma, dma, few, few,
        ],
        compiler_params=pltpu.CompilerParams(
            collective_id=1, has_side_effects=True, vmem_limit_bytes=40 * 1024 * 1024),
    )(u, r, weights, raised, coeff_t)


def place_kernel(ndev, nrows, slots, big, small, rows_out, vec_out, held, in_sem, out_sem):
    bs = held.shape[2]

    def fetch(d):
        return pltpu.make_async_copy(big.at[d], held.at[d], in_sem.at[d])

    def put(d):
        cols = pl.ds(pl.multiple_of(slots[0, d] * bs, bs), bs)
        return pltpu.make_async_copy(held.at[d], rows_out.at[:, cols], out_sem.at[d])

    def loop(action):
        def body(d, carry):
            action(d)
            return carry
        lax.fori_loop(0, ndev, body, 0)

    loop(lambda d: fetch(d).start())
    total = jnp.sum(small[:, 1, :], axis=0, keepdims=True)
    scale = lax.rsqrt(total / nrows + 1e-06)

    def move(d):
        fetch(d).wait()
        put(d).start()
        cols = pl.ds(pl.multiple_of(slots[0, d] * bs, bs), bs)
        vec_out[:, cols] = small[d, 0:1, :] * scale

    loop(move)
    loop(lambda d: put(d).wait())


def place(slot_row, big, small, nrows):
    ndev, keep, bs = big.shape
    vmem = pl.BlockSpec(memory_space=pltpu.VMEM)
    hbm = pl.BlockSpec(memory_space=pl.ANY)
    dma = pltpu.SemaphoreType.DMA((ndev,))
    return pl.pallas_call(
        functools.partial(place_kernel, ndev, nrows),
        out_shape=(
            jax.ShapeDtypeStruct((keep, ndev * bs), jnp.float32),
            jax.ShapeDtypeStruct((1, ndev * bs), jnp.float32),
        ),
        in_specs=[pl.BlockSpec(memory_space=pltpu.SMEM), hbm, vmem],
        out_specs=(hbm, vmem),
        scratch_shapes=[pltpu.VMEM((ndev, keep, bs), jnp.float32), dma, dma],
        compiler_params=pltpu.CompilerParams(vmem_limit_bytes=20 * 1024 * 1024),
    )(slot_row, big, small)


def small_algebra(sums, restart, nrows):
    k = restart.shape[0]
    lower = jnp.linalg.cholesky(sums[:k, :k] / nrows)
    inner = sums[:k, k : k + 1]
    factor = lax.linalg.triangular_solve(lower, restart, left_side=True, lower=True, transpose_a=True)
    half_solve = lax.linalg.triangular_solve(lower, inner, left_side=True, lower=True)
    proj = lax.linalg.triangular_solve(lower, half_solve, left_side=True, lower=True, transpose_a=True) / nrows
    keep = restart.shape[1]
    weights = jnp.concatenate([factor, proj], axis=1).T
    weights = jnp.pad(weights, ((0, round_up(keep + 1, 8) - keep - 1), (0, 0)))
    raised = jnp.dot(lower, restart, precision=HIGHEST)
    return weights, raised.T


def local(u, r, slot_map, restart, coeff):
    ndev = lax.axis_size(AXES)
    ns = lax.axis_size("sub")
    k, keep = restart.shape
    nrows = u.shape[1] * ndev
    deg, _, mloc = coeff.shape
    sums = gram_sums(u, r, ndev, ns)
    weights, raised = small_algebra(sums, restart, nrows)
    coeff_t = coeff.transpose(0, 2, 1).reshape(deg * mloc, k)
    tall = round_up(deg * mloc, 8)
    coeff_t = jnp.pad(coeff_t, ((0, tall - deg * mloc), (0, 0)))
    big, small, turned = exchange(u, r, weights, raised, coeff_t, keep, deg * keep * mloc * ns, ndev, ns)
    rows, vec = place(slot_map, big, small, nrows)
    turned = turned[:, :, : deg * mloc].reshape(ns, keep, deg, mloc)
    new_coeff = turned.transpose(2, 1, 0, 3).reshape(deg, keep, ns * mloc)
    return rows, vec, new_coeff


def solution(mesh):
    P = jax.sharding.PartitionSpec
    in_specs = (P(None, AXES), P(None, AXES), P(AXES, None), P(), P(None, None, "sub"))
    out_specs = (P(None, AXES), P(None, AXES), P())
    return jax.shard_map(local, mesh=mesh, in_specs=in_specs, out_specs=out_specs, check_vma=False)
```

```python
import functools

import jax
import jax.numpy as jnp
from jax import lax
from jax.experimental import pallas as pl
from jax.experimental.pallas import tpu as pltpu

HIGHEST = lax.Precision.HIGHEST
MESH = pl.DeviceIdType.MESH
AXES = ("rows", "sub")
LANES = 128


def round_up(value, unit):
    return -(-value // unit) * unit


def me_of(ns):
    return lax.axis_index("rows") * ns + lax.axis_index("sub")


def greet_all(me, ndev, ns):
    barrier = pltpu.get_barrier_semaphore()

    def greet(o, carry):
        j = (me + o) % ndev
        pl.semaphore_signal(barrier, inc=1, device_id=(j // ns, j % ns), device_id_type=MESH)
        return carry

    lax.fori_loop(1, ndev, greet, 0)
    return barrier


def gram_kernel(ndev, ns, chunk, u_hbm, r_hbm, out_ref, u_ref, r_ref, stage, rs_buf, red, ag_buf,
                in_sem, s1, r1, s2, r2):
    me = me_of(ns)
    pieces = u_ref.shape[1] // chunk
    load_r = pltpu.make_async_copy(r_hbm, r_ref, in_sem.at[pieces])
    load_r.start()
    loads = []
    for c in range(pieces):
        cols = pl.ds(c * chunk, chunk)
        loads.append(pltpu.make_async_copy(u_hbm.at[:, cols], u_ref.at[:, cols], in_sem.at[c]))
        loads[-1].start()
    barrier = greet_all(me, ndev, ns)
    width = out_ref.shape[1]
    pad = width - u_ref.shape[0]
    rpd = width // ndev

    def piece(c, acc):
        loads[c].wait()
        cols = pl.ds(c * chunk, chunk)
        first = lax.broadcasted_iota(jnp.int32, (pad, chunk), 0) == 0
        tail = jnp.where(first, jnp.broadcast_to(r_ref[:, cols], (pad, chunk)), 0.0)
        x = jnp.concatenate([u_ref[:, cols], tail], axis=0)
        hi = x.astype(jnp.bfloat16)
        lo = (x - hi.astype(jnp.float32)).astype(jnp.bfloat16)
        both = jnp.concatenate([hi, lo], axis=0)
        return acc + lax.dot_general(both, both, (((1,), (1,)), ((), ())), preferred_element_type=jnp.float32)

    load_r.wait()
    full = jnp.zeros((2 * width, 2 * width), jnp.float32)
    for c in range(pieces):
        full = piece(c, full)
    cross = full[:width, width:]
    gram = full[:width, :width] + (cross + cross.T) + full[width:, width:]
    for i in range(ndev):
        stage[i] = gram[i * rpd : (i + 1) * rpd, :]
    rs_buf[me] = stage[me]
    pl.semaphore_wait(barrier, ndev - 1)

    def scatter_copy(j, slot):
        return pltpu.make_async_remote_copy(
            src_ref=stage.at[j], dst_ref=rs_buf.at[slot], send_sem=s1.at[j], recv_sem=r1.at[slot],
            device_id=(j // ns, j % ns), device_id_type=MESH)

    def gather_copy(j, slot):
        return pltpu.make_async_remote_copy(
            src_ref=red, dst_ref=ag_buf.at[slot], send_sem=s2.at[j], recv_sem=r2.at[slot],
            device_id=(j // ns, j % ns), device_id_type=MESH)

    def loop(action):
        def body(o, carry):
            action((me + o) % ndev)
            return carry
        lax.fori_loop(1, ndev, body, 0)

    loop(lambda j: scatter_copy(j, me).start())
    loop(lambda j: scatter_copy(j, j).wait_recv())
    total = jnp.sum(rs_buf[...], axis=0)
    red[...] = total
    ag_buf[me] = total
    loop(lambda j: gather_copy(j, me).start())
    loop(lambda j: gather_copy(j, j).wait_recv())
    for i in range(ndev):
        out_ref[i * rpd : (i + 1) * rpd, :] = ag_buf[i]
    loop(lambda j: scatter_copy(j, me).wait_send())
    loop(lambda j: gather_copy(j, me).wait_send())


def gram_sums(u, r, ndev, ns):
    width = LANES
    rpd = width // ndev
    chunk = min(2048, u.shape[1])
    dma = pltpu.SemaphoreType.DMA((ndev,))
    vmem = pl.BlockSpec(memory_space=pltpu.VMEM)
    hbm = pl.BlockSpec(memory_space=pltpu.MemorySpace.HBM)
    return pl.pallas_call(
        functools.partial(gram_kernel, ndev, ns, chunk),
        out_shape=jax.ShapeDtypeStruct((width, width), jnp.float32),
        in_specs=[hbm, hbm],
        out_specs=vmem,
        scratch_shapes=[
            pltpu.VMEM(u.shape, jnp.float32),
            pltpu.VMEM(r.shape, jnp.float32),
            pltpu.VMEM((ndev, rpd, width), jnp.float32),
            pltpu.VMEM((ndev, rpd, width), jnp.float32),
            pltpu.VMEM((rpd, width), jnp.float32),
            pltpu.VMEM((ndev, rpd, width), jnp.float32),
            pltpu.SemaphoreType.DMA((u.shape[1] // chunk + 1,)),
            dma, dma, dma, dma,
        ],
        compiler_params=pltpu.CompilerParams(
            collective_id=0, has_side_effects=True, vmem_limit_bytes=60 * 1024 * 1024),
    )(u, r)


def factor_panels(sums_ref, restart_ref, work, upper, nrows, panel):
    k, keep = restart_ref.shape
    width = sums_ref.shape[1]
    row = lax.broadcasted_iota(jnp.int32, (width, width), 0)
    lane = lax.broadcasted_iota(jnp.int32, (width, width), 1)
    line = lax.broadcasted_iota(jnp.int32, (1, width), 1)
    work[:, :width] = sums_ref[...] * (1.0 / nrows)
    work[:, width:] = jnp.where(row == lane, 1.0, 0.0)
    upper[...] = jnp.zeros_like(upper)

    def step(i, carry):
        base = i * panel
        rows = [work[pl.ds(base + a, 1), :] for a in range(panel)]
        left = work[:, :width]
        cols = [jnp.sum(jnp.where(lane == base + a, left, 0.0), axis=1, keepdims=True) for a in range(panel)]
        block = {
            (a, b): jnp.sum(jnp.where(line == base + b, rows[a][:, :width], 0.0), axis=1, keepdims=True)
            for a in range(panel) for b in range(a, panel)
        }
        for a in range(panel):
            inverse = 1.0 / block[a, a]
            for b in range(a + 1, panel):
                ratio = block[a, b] * inverse
                rows[b] = rows[b] - ratio * rows[a]
                cols[b] = cols[b] - ratio * cols[a]
                for c in range(b, panel):
                    block[b, c] = block[b, c] - ratio * block[a, c]
            cols[a] = (cols[a], inverse)
            upper[pl.ds(base + a, 1), :] = rows[a] * lax.rsqrt(block[a, a])
        work[...] = work[...] - sum((cols[a][0] * cols[a][1]) * rows[a] for a in range(panel))
        return carry

    lax.fori_loop(0, k // panel, step, 0)
    turned = restart_ref[...].T
    both = jnp.dot(turned, upper[:k, :], precision=HIGHEST, preferred_element_type=jnp.float32)
    half = upper[:, :width].T[k : k + 8, :]
    proj = jnp.dot(half, upper[:, width:], precision=HIGHEST, preferred_element_type=jnp.float32)
    raised = both[:, :k]
    weights = jnp.concatenate([both[:, width:], proj], axis=0)[:, :k]
    return weights, raised


def exchange_kernel(ndev, ns, keep, count, nrows, u_hbm, r_hbm, sums_ref, restart_ref, coeff_ref,
                    big_out, small_out, coeff_out, u_ref, r_ref, work, upper, load_sem, send, small, cg, own_sem,
                    s1, r1, s2, r2, s3, r3):
    r, s = lax.axis_index("rows"), lax.axis_index("sub")
    me = r * ns + s
    nr = ndev // ns
    bs = send.shape[2]
    load_u = pltpu.make_async_copy(u_hbm, u_ref, load_sem.at[0])
    load_r = pltpu.make_async_copy(r_hbm, r_ref, load_sem.at[1])
    load_u.start()
    load_r.start()
    barrier = greet_all(me, ndev, ns)

    def coeff_copy(t, slot):
        return pltpu.make_async_remote_copy(
            src_ref=coeff_ref, dst_ref=cg.at[slot], send_sem=s3.at[t], recv_sem=r3.at[slot],
            device_id=(r, t), device_id_type=MESH)

    def big_copy(j, slot):
        return pltpu.make_async_remote_copy(
            src_ref=send.at[j], dst_ref=big_out.at[slot], send_sem=s1.at[j], recv_sem=r1.at[slot],
            device_id=(j // ns, j % ns), device_id_type=MESH)

    def small_copy(j, slot):
        return pltpu.make_async_remote_copy(
            src_ref=small.at[j], dst_ref=small_out.at[slot], send_sem=s2.at[j], recv_sem=r2.at[slot],
            device_id=(j // ns, j % ns), device_id_type=MESH)

    def loop(action):
        def body(o, carry):
            action((me + o) % ndev)
            return carry
        lax.fori_loop(1, ndev, body, 0)

    panel = next(p for p in (4, 2, 1) if restart_ref.shape[0] % p == 0)
    weights, raised = factor_panels(sums_ref, restart_ref, work, upper, nrows, panel)
    load_u.wait()
    load_r.wait()
    half = ns // 2
    side, pos = s // half, s % half
    across = [(1 - side) * half + (pos + q) % half for q in range(half)]
    beside = [side * half + (pos + q) % half for q in range(half)]
    order = []
    for q in range(half):
        order += [across[q], beside[half - 1 - q]]

    def step(d, acc):
        targets = [((r + d) % nr) * ns + t for t in order]
        for j in targets:
            cols = pl.ds(pl.multiple_of(j * bs, bs), bs)
            y = jnp.dot(weights, u_ref[:, cols], precision=HIGHEST, preferred_element_type=jnp.float32)
            rest = r_ref[:, cols] - y[keep : keep + 1, :]
            send[j] = y[:keep, :]
            small[j, 0:1, :] = rest
            acc = acc + rest * rest

        @pl.when(d == 0)
        def _():
            pl.semaphore_wait(barrier, ndev - 1)

        for j in targets:
            @pl.when(j != me)
            def _():
                big_copy(j, me).start()

        return acc

    acc = lax.fori_loop(0, nr, step, jnp.zeros((1, bs), jnp.float32))
    partial = jnp.sum(acc, axis=1, keepdims=True)

    def mark(j, carry):
        small[j, 1:2, :] = jnp.broadcast_to(partial, (1, bs))
        return carry

    lax.fori_loop(0, ndev, mark, 0)
    own_big = pltpu.make_async_copy(send.at[me], big_out.at[me], own_sem.at[0])
    own_small = pltpu.make_async_copy(small.at[me], small_out.at[me], own_sem.at[1])
    own_big.start()
    own_small.start()
    for o in range(1, ns):
        coeff_copy((s + o) % ns, s).start()
    loop(lambda j: small_copy(j, me).start())
    cg[s] = coeff_ref[...]
    for o in range(1, ns):
        coeff_copy((s + o) % ns, (s + o) % ns).wait_recv()
    turned = [
        lax.dot_general(raised, cg[t], (((1,), (1,)), ((), ())), precision=HIGHEST,
                        preferred_element_type=jnp.float32)
        for t in range(ns)
    ]
    squares = sum(jnp.sum(part * part) for part in turned)
    scale = lax.rsqrt(jnp.full((1, 1), squares / count + 1e-06, jnp.float32))
    for t in range(ns):
        coeff_out[t] = turned[t] * scale
    own_big.wait()
    own_small.wait()
    loop(lambda j: big_copy(j, j).wait_recv())
    loop(lambda j: small_copy(j, j).wait_recv())
    loop(lambda j: big_copy(j, me).wait_send())
    loop(lambda j: small_copy(j, me).wait_send())
    for o in range(1, ns):
        coeff_copy((s + o) % ns, s).wait_send()


def exchange(u, r, sums, restart, coeff_t, keep, count, ndev, ns):
    bs = u.shape[1] // ndev
    vmem = pl.BlockSpec(memory_space=pltpu.VMEM)
    hbm = pl.BlockSpec(memory_space=pltpu.MemorySpace.HBM)
    dma = pltpu.SemaphoreType.DMA((ndev,))
    few = pltpu.SemaphoreType.DMA((ns,))
    f32 = jnp.float32
    return pl.pallas_call(
        functools.partial(exchange_kernel, ndev, ns, keep, count, u.shape[1] * ndev),
        out_shape=(
            jax.ShapeDtypeStruct((ndev, keep, bs), f32),
            jax.ShapeDtypeStruct((ndev, 2, bs), f32),
            jax.ShapeDtypeStruct((ns, keep, coeff_t.shape[0]), f32),
        ),
        in_specs=[hbm, hbm, vmem, vmem, vmem],
        out_specs=(hbm, hbm, vmem),
        scratch_shapes=[
            pltpu.VMEM(u.shape, f32),
            pltpu.VMEM(r.shape, f32),
            pltpu.VMEM((sums.shape[0], 2 * sums.shape[1]), f32),
            pltpu.VMEM((sums.shape[0], 2 * sums.shape[1]), f32),
            pltpu.SemaphoreType.DMA((2,)),
            pltpu.VMEM((ndev, keep, bs), f32),
            pltpu.VMEM((ndev, 2, bs), f32),
            pltpu.VMEM((ns,) + coeff_t.shape, f32),
            pltpu.SemaphoreType.DMA((2,)),
            dma, dma, dma, dma, few, few,
        ],
        compiler_params=pltpu.CompilerParams(
            collective_id=1, has_side_effects=True, vmem_limit_bytes=60 * 1024 * 1024),
    )(u, r, sums, restart, coeff_t)


def place_kernel(ndev, nrows, slots, big, small, rows_out, vec_out, held, in_sem, out_sem):
    bs = held.shape[2]

    def fetch(d):
        return pltpu.make_async_copy(big.at[d], held.at[d], in_sem.at[d])

    def put(d):
        cols = pl.ds(pl.multiple_of(slots[0, d] * bs, bs), bs)
        return pltpu.make_async_copy(held.at[d], rows_out.at[:, cols], out_sem.at[d])

    def loop(action):
        def body(d, carry):
            action(d)
            return carry
        lax.fori_loop(0, ndev, body, 0)

    loop(lambda d: fetch(d).start())
    total = jnp.sum(small[:, 1, :], axis=0, keepdims=True)
    scale = lax.rsqrt(total / nrows + 1e-06)

    def move(d):
        fetch(d).wait()
        put(d).start()
        cols = pl.ds(pl.multiple_of(slots[0, d] * bs, bs), bs)
        vec_out[:, cols] = small[d, 0:1, :] * scale

    loop(move)
    loop(lambda d: put(d).wait())


def place(slot_row, big, small, nrows):
    ndev, keep, bs = big.shape
    vmem = pl.BlockSpec(memory_space=pltpu.VMEM)
    hbm = pl.BlockSpec(memory_space=pl.ANY)
    dma = pltpu.SemaphoreType.DMA((ndev,))
    return pl.pallas_call(
        functools.partial(place_kernel, ndev, nrows),
        out_shape=(
            jax.ShapeDtypeStruct((keep, ndev * bs), jnp.float32),
            jax.ShapeDtypeStruct((1, ndev * bs), jnp.float32),
        ),
        in_specs=[pl.BlockSpec(memory_space=pltpu.SMEM), hbm, vmem],
        out_specs=(hbm, vmem),
        scratch_shapes=[pltpu.VMEM((ndev, keep, bs), jnp.float32), dma, dma],
        compiler_params=pltpu.CompilerParams(vmem_limit_bytes=20 * 1024 * 1024),
    )(slot_row, big, small)


def local(u, r, slot_map, restart, coeff):
    ndev = lax.axis_size(AXES)
    ns = lax.axis_size("sub")
    k, keep = restart.shape
    nrows = u.shape[1] * ndev
    deg, _, mloc = coeff.shape
    sums = gram_sums(u, r, ndev, ns)
    coeff_t = coeff.transpose(0, 2, 1).reshape(deg * mloc, k)
    tall = round_up(deg * mloc, 8)
    coeff_t = jnp.pad(coeff_t, ((0, tall - deg * mloc), (0, 0)))
    big, small, turned = exchange(u, r, sums, restart, coeff_t, keep, deg * keep * mloc * ns, ndev, ns)
    rows, vec = place(slot_map, big, small, nrows)
    turned = turned[:, :, : deg * mloc].reshape(ns, keep, deg, mloc)
    new_coeff = turned.transpose(2, 1, 0, 3).reshape(deg, keep, ns * mloc)
    return rows, vec, new_coeff


def solution(mesh):
    P = jax.sharding.PartitionSpec
    in_specs = (P(None, AXES), P(None, AXES), P(AXES, None), P(), P(None, None, "sub"))
    out_specs = (P(None, AXES), P(None, AXES), P())
    return jax.shard_map(local, mesh=mesh, in_specs=in_specs, out_specs=out_specs, check_vma=False)
```

```python
import functools

import jax
import jax.numpy as jnp
from jax import lax
from jax.experimental import pallas as pl
from jax.experimental.pallas import tpu as pltpu

HIGHEST = lax.Precision.HIGHEST
MESH = pl.DeviceIdType.MESH
AXES = ("rows", "sub")
LANES = 128


def me_of(ns):
    return lax.axis_index("rows") * ns + lax.axis_index("sub")


def greet_all(me, ndev, ns):
    barrier = pltpu.get_barrier_semaphore()

    def greet(o, carry):
        j = (me + o) % ndev
        pl.semaphore_signal(barrier, inc=1, device_id=(j // ns, j % ns), device_id_type=MESH)
        return carry

    lax.fori_loop(1, ndev, greet, 0)
    return barrier


def gram_kernel(ndev, ns, chunk, u_hbm, r_hbm, out_ref, u_ref, r_ref, stage, rs_buf, red, ag_buf,
                in_sem, s1, r1, s2, r2):
    me = me_of(ns)
    pieces = u_ref.shape[1] // chunk
    load_r = pltpu.make_async_copy(r_hbm, r_ref, in_sem.at[pieces])
    load_r.start()
    loads = []
    for c in range(pieces):
        cols = pl.ds(c * chunk, chunk)
        loads.append(pltpu.make_async_copy(u_hbm.at[:, cols], u_ref.at[:, cols], in_sem.at[c]))
        loads[-1].start()
    barrier = greet_all(me, ndev, ns)
    width = out_ref.shape[1]
    pad = width - u_ref.shape[0]
    rpd = width // ndev

    def piece(c, acc):
        loads[c].wait()
        cols = pl.ds(c * chunk, chunk)
        first = lax.broadcasted_iota(jnp.int32, (pad, chunk), 0) == 0
        tail = jnp.where(first, jnp.broadcast_to(r_ref[:, cols], (pad, chunk)), 0.0)
        x = jnp.concatenate([u_ref[:, cols], tail], axis=0)
        hi = x.astype(jnp.bfloat16)
        lo = (x - hi.astype(jnp.float32)).astype(jnp.bfloat16)
        both = jnp.concatenate([hi, lo], axis=0)
        return acc + lax.dot_general(both, both, (((1,), (1,)), ((), ())), preferred_element_type=jnp.float32)

    load_r.wait()
    full = jnp.zeros((2 * width, 2 * width), jnp.float32)
    for c in range(pieces):
        full = piece(c, full)
    cross = full[:width, width:]
    gram = full[:width, :width] + (cross + cross.T) + full[width:, width:]
    for i in range(ndev):
        stage[i] = gram[i * rpd : (i + 1) * rpd, :]
    rs_buf[me] = stage[me]
    pl.semaphore_wait(barrier, ndev - 1)

    def scatter_copy(j, slot):
        return pltpu.make_async_remote_copy(
            src_ref=stage.at[j], dst_ref=rs_buf.at[slot], send_sem=s1.at[j], recv_sem=r1.at[slot],
            device_id=(j // ns, j % ns), device_id_type=MESH)

    def gather_copy(j, slot):
        return pltpu.make_async_remote_copy(
            src_ref=red, dst_ref=ag_buf.at[slot], send_sem=s2.at[j], recv_sem=r2.at[slot],
            device_id=(j // ns, j % ns), device_id_type=MESH)

    def loop(action):
        def body(o, carry):
            action((me + o) % ndev)
            return carry
        lax.fori_loop(1, ndev, body, 0)

    loop(lambda j: scatter_copy(j, me).start())
    loop(lambda j: scatter_copy(j, j).wait_recv())
    total = jnp.sum(rs_buf[...], axis=0)
    red[...] = total
    ag_buf[me] = total
    loop(lambda j: gather_copy(j, me).start())
    loop(lambda j: gather_copy(j, j).wait_recv())
    for i in range(ndev):
        out_ref[i * rpd : (i + 1) * rpd, :] = ag_buf[i]
    loop(lambda j: scatter_copy(j, me).wait_send())
    loop(lambda j: gather_copy(j, me).wait_send())


def gram_sums(u, r, ndev, ns):
    width = LANES
    rpd = width // ndev
    chunk = min(2048, u.shape[1])
    dma = pltpu.SemaphoreType.DMA((ndev,))
    vmem = pl.BlockSpec(memory_space=pltpu.VMEM)
    hbm = pl.BlockSpec(memory_space=pltpu.MemorySpace.HBM)
    return pl.pallas_call(
        functools.partial(gram_kernel, ndev, ns, chunk),
        out_shape=jax.ShapeDtypeStruct((width, width), jnp.float32),
        in_specs=[hbm, hbm],
        out_specs=vmem,
        scratch_shapes=[
            pltpu.VMEM(u.shape, jnp.float32),
            pltpu.VMEM(r.shape, jnp.float32),
            pltpu.VMEM((ndev, rpd, width), jnp.float32),
            pltpu.VMEM((ndev, rpd, width), jnp.float32),
            pltpu.VMEM((rpd, width), jnp.float32),
            pltpu.VMEM((ndev, rpd, width), jnp.float32),
            pltpu.SemaphoreType.DMA((u.shape[1] // chunk + 1,)),
            dma, dma, dma, dma,
        ],
        compiler_params=pltpu.CompilerParams(
            collective_id=0, has_side_effects=True, vmem_limit_bytes=60 * 1024 * 1024),
    )(u, r)


def factor_panels(sums_ref, restart_ref, work, upper, nrows, panel):
    keep, k = restart_ref.shape
    width = sums_ref.shape[1]
    row = lax.broadcasted_iota(jnp.int32, (width, width), 0)
    lane = lax.broadcasted_iota(jnp.int32, (width, width), 1)
    line = lax.broadcasted_iota(jnp.int32, (1, width), 1)
    work[:, :width] = sums_ref[...] * (1.0 / nrows)
    work[:, width:] = jnp.where(row == lane, 1.0, 0.0)
    upper[...] = jnp.zeros_like(upper)

    def step(i, carry):
        base = i * panel
        rows = [work[pl.ds(base + a, 1), :] for a in range(panel)]
        left = work[:, :width]
        cols = [jnp.sum(jnp.where(lane == base + a, left, 0.0), axis=1, keepdims=True) for a in range(panel)]
        block = {
            (a, b): jnp.sum(jnp.where(line == base + b, rows[a][:, :width], 0.0), axis=1, keepdims=True)
            for a in range(panel) for b in range(a, panel)
        }
        for a in range(panel):
            inverse = 1.0 / block[a, a]
            for b in range(a + 1, panel):
                ratio = block[a, b] * inverse
                rows[b] = rows[b] - ratio * rows[a]
                cols[b] = cols[b] - ratio * cols[a]
                for c in range(b, panel):
                    block[b, c] = block[b, c] - ratio * block[a, c]
            cols[a] = (cols[a], inverse)
            upper[pl.ds(base + a, 1), :] = rows[a] * lax.rsqrt(block[a, a])
        work[...] = work[...] - sum((cols[a][0] * cols[a][1]) * rows[a] for a in range(panel))
        return carry

    lax.fori_loop(0, k // panel, step, 0)
    both = jnp.dot(restart_ref[...], upper[:k, :], precision=HIGHEST, preferred_element_type=jnp.float32)
    half = upper[:, :width].T[k : k + 8, :]
    proj = jnp.dot(half, upper[:, width:], precision=HIGHEST, preferred_element_type=jnp.float32)
    raised = both[:, :k]
    weights = jnp.concatenate([both[:, width:], proj], axis=0)[:, :k]
    return weights, raised


def exchange_kernel(ndev, ns, keep, count, nrows, u_hbm, r_hbm, sums_ref, restart_ref, coeff_ref,
                    big_out, small_out, coeff_out, u_ref, r_ref, work, upper, load_sem, send, small, cg, own_sem,
                    s1, r1, s2, r2, s3, r3):
    r, s = lax.axis_index("rows"), lax.axis_index("sub")
    me = r * ns + s
    nr = ndev // ns
    bs = send.shape[2]
    load_u = pltpu.make_async_copy(u_hbm, u_ref, load_sem.at[0])
    load_r = pltpu.make_async_copy(r_hbm, r_ref, load_sem.at[1])
    load_u.start()
    load_r.start()
    barrier = greet_all(me, ndev, ns)

    def coeff_copy(t, slot):
        return pltpu.make_async_remote_copy(
            src_ref=coeff_ref, dst_ref=cg.at[slot], send_sem=s3.at[t], recv_sem=r3.at[slot],
            device_id=(r, t), device_id_type=MESH)

    def big_copy(j, slot):
        return pltpu.make_async_remote_copy(
            src_ref=send.at[j], dst_ref=big_out.at[slot], send_sem=s1.at[j], recv_sem=r1.at[slot],
            device_id=(j // ns, j % ns), device_id_type=MESH)

    def small_copy(j, slot):
        return pltpu.make_async_remote_copy(
            src_ref=small.at[j], dst_ref=small_out.at[slot], send_sem=s2.at[j], recv_sem=r2.at[slot],
            device_id=(j // ns, j % ns), device_id_type=MESH)

    def loop(action):
        def body(o, carry):
            action((me + o) % ndev)
            return carry
        lax.fori_loop(1, ndev, body, 0)

    panel = next(p for p in (4, 2, 1) if restart_ref.shape[1] % p == 0)
    weights, raised = factor_panels(sums_ref, restart_ref, work, upper, nrows, panel)
    load_u.wait()
    load_r.wait()
    half = ns // 2
    side, pos = s // half, s % half
    across = [(1 - side) * half + (pos + q) % half for q in range(half)]
    beside = [side * half + (pos + q) % half for q in range(half)]
    order = []
    for q in range(half):
        order += [across[q], beside[half - 1 - q]]

    def step(d, acc):
        targets = [((r + d) % nr) * ns + t for t in order]
        for j in targets:
            cols = pl.ds(pl.multiple_of(j * bs, bs), bs)
            y = jnp.dot(weights, u_ref[:, cols], precision=HIGHEST, preferred_element_type=jnp.float32)
            rest = r_ref[:, cols] - y[keep : keep + 1, :]
            send[j] = y[:keep, :]
            small[j, 0:1, :] = rest
            acc = acc + rest * rest

        @pl.when(d == 0)
        def _():
            pl.semaphore_wait(barrier, ndev - 1)

        for j in targets:
            @pl.when(j != me)
            def _():
                big_copy(j, me).start()

        return acc

    acc = lax.fori_loop(0, nr, step, jnp.zeros((1, bs), jnp.float32))
    partial = jnp.sum(acc, axis=1, keepdims=True)

    def mark(j, carry):
        small[j, 1:2, :] = jnp.broadcast_to(partial, (1, bs))
        return carry

    lax.fori_loop(0, ndev, mark, 0)
    own_big = pltpu.make_async_copy(send.at[me], big_out.at[me], own_sem.at[0])
    own_small = pltpu.make_async_copy(small.at[me], small_out.at[me], own_sem.at[1])
    own_big.start()
    own_small.start()
    for o in range(1, ns):
        coeff_copy((s + o) % ns, s).start()
    loop(lambda j: small_copy(j, me).start())
    cg[s] = coeff_ref[...]
    for o in range(1, ns):
        coeff_copy((s + o) % ns, (s + o) % ns).wait_recv()
    deg, mloc, _ = coeff_ref.shape
    turned = [
        jnp.concatenate(
            [
                lax.dot_general(raised, cg[t, i], (((1,), (1,)), ((), ())), precision=HIGHEST,
                                preferred_element_type=jnp.float32)
                for t in range(ns)
            ],
            axis=1,
        )
        for i in range(deg)
    ]
    squares = sum(jnp.sum(part * part) for part in turned)
    scale = lax.rsqrt(jnp.full((1, 1), squares / count + 1e-06, jnp.float32))
    for i in range(deg):
        coeff_out[i] = turned[i] * scale
    own_big.wait()
    own_small.wait()
    loop(lambda j: big_copy(j, j).wait_recv())
    loop(lambda j: small_copy(j, j).wait_recv())
    loop(lambda j: big_copy(j, me).wait_send())
    loop(lambda j: small_copy(j, me).wait_send())
    for o in range(1, ns):
        coeff_copy((s + o) % ns, s).wait_send()


def exchange(u, r, sums, restart, coeff_t, keep, count, ndev, ns):
    bs = u.shape[1] // ndev
    vmem = pl.BlockSpec(memory_space=pltpu.VMEM)
    hbm = pl.BlockSpec(memory_space=pltpu.MemorySpace.HBM)
    dma = pltpu.SemaphoreType.DMA((ndev,))
    few = pltpu.SemaphoreType.DMA((ns,))
    f32 = jnp.float32
    return pl.pallas_call(
        functools.partial(exchange_kernel, ndev, ns, keep, count, u.shape[1] * ndev),
        out_shape=(
            jax.ShapeDtypeStruct((ndev, keep, bs), f32),
            jax.ShapeDtypeStruct((ndev, 2, bs), f32),
            jax.ShapeDtypeStruct((coeff_t.shape[0], keep, ns * coeff_t.shape[1]), f32),
        ),
        in_specs=[hbm, hbm, vmem, vmem, vmem],
        out_specs=(hbm, hbm, vmem),
        scratch_shapes=[
            pltpu.VMEM(u.shape, f32),
            pltpu.VMEM(r.shape, f32),
            pltpu.VMEM((sums.shape[0], 2 * sums.shape[1]), f32),
            pltpu.VMEM((sums.shape[0], 2 * sums.shape[1]), f32),
            pltpu.SemaphoreType.DMA((2,)),
            pltpu.VMEM((ndev, keep, bs), f32),
            pltpu.VMEM((ndev, 2, bs), f32),
            pltpu.VMEM((ns,) + coeff_t.shape, f32),
            pltpu.SemaphoreType.DMA((2,)),
            dma, dma, dma, dma, few, few,
        ],
        compiler_params=pltpu.CompilerParams(
            collective_id=1, has_side_effects=True, vmem_limit_bytes=60 * 1024 * 1024),
    )(u, r, sums, restart, coeff_t)


def place_kernel(ndev, nrows, slots, big, small_hbm, rows_out, vec_out, held, small, in_sem, out_sem, small_sem):
    bs = held.shape[2]
    load_small = pltpu.make_async_copy(small_hbm, small, small_sem.at[0])

    def fetch(d):
        return pltpu.make_async_copy(big.at[d], held.at[d], in_sem.at[d])

    def put(d):
        cols = pl.ds(pl.multiple_of(slots[0, d] * bs, bs), bs)
        return pltpu.make_async_copy(held.at[d], rows_out.at[:, cols], out_sem.at[d])

    def loop(action):
        def body(d, carry):
            action(d)
            return carry
        lax.fori_loop(0, ndev, body, 0)

    loop(lambda d: fetch(d).start())
    load_small.start()

    def move(d):
        fetch(d).wait()
        put(d).start()

    loop(move)
    load_small.wait()
    total = jnp.sum(small[:, 1, :], axis=0, keepdims=True)
    scale = lax.rsqrt(total / nrows + 1e-06)
    for d in range(ndev):
        cols = pl.ds(pl.multiple_of(slots[0, d] * bs, bs), bs)
        vec_out[:, cols] = small[d, 0:1, :] * scale
    loop(lambda d: put(d).wait())


def place(slot_row, big, small, nrows):
    ndev, keep, bs = big.shape
    vmem = pl.BlockSpec(memory_space=pltpu.VMEM)
    hbm = pl.BlockSpec(memory_space=pltpu.MemorySpace.HBM)
    dma = pltpu.SemaphoreType.DMA((ndev,))
    return pl.pallas_call(
        functools.partial(place_kernel, ndev, nrows),
        out_shape=(
            jax.ShapeDtypeStruct((keep, ndev * bs), jnp.float32),
            jax.ShapeDtypeStruct((1, ndev * bs), jnp.float32),
        ),
        in_specs=[pl.BlockSpec(memory_space=pltpu.SMEM), hbm, hbm],
        out_specs=(hbm, vmem),
        scratch_shapes=[
            pltpu.VMEM(big.shape, jnp.float32),
            pltpu.VMEM(small.shape, jnp.float32),
            dma, dma, pltpu.SemaphoreType.DMA((1,)),
        ],
        compiler_params=pltpu.CompilerParams(vmem_limit_bytes=60 * 1024 * 1024),
    )(slot_row, big, small)


def local(u, r, slot_map, restart, coeff):
    ndev = lax.axis_size(AXES)
    ns = lax.axis_size("sub")
    k, keep = restart.shape
    nrows = u.shape[1] * ndev
    deg, _, mloc = coeff.shape
    sums = gram_sums(u, r, ndev, ns)
    coeff_t = coeff.transpose(0, 2, 1)
    big, small, new_coeff = exchange(u, r, sums, restart.T, coeff_t, keep, deg * keep * mloc * ns, ndev, ns)
    rows, vec = place(slot_map, big, small, nrows)
    return rows, vec, new_coeff


def solution(mesh):
    P = jax.sharding.PartitionSpec
    in_specs = (P(None, AXES), P(None, AXES), P(AXES, None), P(), P(None, None, "sub"))
    out_specs = (P(None, AXES), P(None, AXES), P())
    return jax.shard_map(local, mesh=mesh, in_specs=in_specs, out_specs=out_specs, check_vma=False)
```
